32 devices in a mesh: gx: 4 (over z), gy: 4 (over x, core), gz: 2 (over y).
Axes of the slice: x: 2, y: 2, z: 4, core: 2. Of those that a mesh axis runs over, the one named last changes fastest.
Arguments:
- hidden_in: bfloat16 [2048, 4096], P(('gx', 'gy'), 'gz'), may hold values from -40 to 40
- norm_gain: float32 [4096], P('gz'), may hold values from 0.25 to 1.75
- normed_grad: bfloat16 [2048, 4096], P(('gx', 'gy'), 'gz'), may hold values from -64 to 64
- key_grad: bfloat16 [2048, 512], P(('gx', 'gy')), may hold values from -6 to 6
- weight_blocks: bfloat16 [16, 2, 520, 128], P(('gx', 'gy'), 'gz'), may hold values from -0.09375 to 0.09375
- block_count: int32 [2, 16], P('gz'), may hold values from 1 to 520, as said below
Outputs:
- hidden_grad: bfloat16 [2048, 4096], P(('gx', 'gy'), 'gz')
- weight_grad: float32 [16, 2, 520, 128], P(('gx', 'gy'), 'gz')
The draws below stay inside these ranges and needn't reach their ends.
Inputs may be any that keep to these rules, and one draw needn't show every extreme that they name: `block_count`: each row sums to 8192; in each row the owners i * 4 to i * 4 + 3 hold together exactly the blocks i * 2048 to min((i + 1) * 2048, 8192) - 1, and one of them holds exactly 520 blocks.
All inputs are finite; a program needn't handle non-finite values.
Results may differ from the reference program's by a relative error of at most 0.0029.
Values may be sent and summed in bfloat16 or wider, within the bound.
No kernel may reach another device: no remote copies, remote signals or barrier semaphores. Data moves between devices by JAX's collectives and lax.ppermute only.
A program may use at most 64 MiB of HBM per device.

```python
import math
import jax
import jax.numpy as jnp
from jax import lax

D = 4096
KVW = 512
TOK_DEV = 128
OUTER = 4
INNER = 4
OWNERS = 16
TOKENS = 2048
QUARTERS = 2
BLOCKS = 8192
GROUPB = 2048
MAXB = 520


def joint_activations(key):
    subkeys = jax.random.split(jax.random.fold_in(key, 7001), 5)
    position = jnp.arange(D, dtype=jnp.float32) / D
    base = jnp.clip(jax.random.normal(subkeys[0], (TOKENS, D), jnp.float32), -4.0, 4.0)
    column = jnp.power(3.0, position) * jnp.exp(jax.random.uniform(subkeys[1], (D,), jnp.float32, math.log(0.6), math.log(1.6)))
    hidden = base * column[None, :]
    coefficient = jax.random.uniform(subkeys[3], (TOKENS, 1), jnp.float32, -1.5, 1.5)
    noise = 0.5 * jnp.clip(jax.random.normal(subkeys[4], (TOKENS, D), jnp.float32), -4.0, 4.0)
    return (hidden, coefficient * hidden + noise)


def draw_hidden_in(key, part):
    hidden, _ = joint_activations(key)
    return hidden.astype(jnp.bfloat16)


def draw_normed_grad(key, part):
    _, cotangent = joint_activations(key)
    return cotangent.astype(jnp.bfloat16)


def draw_block_count(key, part):
    subkeys = jax.random.split(jax.random.fold_in(key, 7002), 2)
    group_ids = jnp.arange(OUTER, dtype=jnp.int32)
    totals = jnp.minimum(GROUPB, BLOCKS - group_ids * GROUPB).astype(jnp.int32)
    totals = jnp.broadcast_to(totals[None, :, None], (QUARTERS, OUTER, 1))
    chosen = jax.random.randint(subkeys[0], (QUARTERS, OUTER, 1), 0, INNER, dtype=jnp.int32)
    member = jnp.arange(INNER, dtype=jnp.int32)[None, None, :]
    is_full = member == chosen
    raw_weight = jax.random.randint(subkeys[1], (QUARTERS, OUTER, INNER), 1, 6, dtype=jnp.int32)
    weights = jnp.where(is_full, 0, raw_weight * raw_weight * raw_weight)
    extra = totals - MAXB - (INNER - 1)
    share = extra * weights // jnp.sum(weights, axis=2, keepdims=True)
    share = jnp.minimum(share, MAXB - 1)
    leftover = extra - jnp.sum(share, axis=2, keepdims=True)
    room = jnp.where(is_full, 0, MAXB - 1 - share)
    before = jnp.cumsum(room, axis=2) - room
    share = share + jnp.clip(leftover - before, 0, room)
    counts = jnp.where(is_full, MAXB, 1 + share)
    return counts.reshape(QUARTERS, OWNERS).astype(jnp.int32)


def block_levels(stream_key, dims, cuts, low, largest):
    factor_of = 1.0
    for dim, blocks in cuts:
        steps = jax.random.uniform(jax.random.fold_in(jax.random.fold_in(stream_key, 6), dim), (blocks,), jnp.float32, low / len(cuts), largest / len(cuts))
        factor_of = factor_of * jnp.repeat(jnp.exp(steps), dims[dim] // blocks).reshape((-1,) + (1,) * (len(dims) - 1 - dim))
    return factor_of


def scatter_about(rng, dims, deviation, most, cuts=(), held_as=jnp.bfloat16):
    loudness = block_levels(rng, dims, cuts, -0.22, 0.18) if cuts else 1.0
    result = jax.random.normal(rng, dims, jnp.float32) * deviation * loudness
    return jnp.minimum(jnp.maximum(result, -most), most).astype(held_as)


def setup_inputs(seed: int = 0) -> dict:
    seeds = jax.random.split(jax.random.key(seed), 7)
    return {
        "hidden_in": draw_hidden_in(jax.random.fold_in(seeds[6], 71), 0),
        "norm_gain": jnp.clip(1.0 + 0.15 * jax.random.normal(seeds[1], (D,), jnp.float32), 0.25, 1.75),
        "normed_grad": draw_normed_grad(jax.random.fold_in(seeds[6], 71), 0),
        "key_grad": scatter_about(seeds[3], (TOKENS, KVW), 1.0, 6.0, ((0, 16),)),
        "weight_blocks": scatter_about(seeds[4], (OWNERS, QUARTERS, MAXB, 128), D ** -0.5, 0.09375, ((0, 16), (1, 2))),
        "block_count": draw_block_count(jax.random.fold_in(seeds[6], 71), 0),
    }


EPS = 1e-06

def block_layout(counts):
    ends = jnp.cumsum(counts).astype(jnp.int32)
    starts = (ends - counts).astype(jnp.int32)
    block_ids = jnp.arange(BLOCKS, dtype=jnp.int32)
    owner = jnp.searchsorted(ends, block_ids, side='right').astype(jnp.int32)
    gather_index = (owner * MAXB + block_ids - starts[owner]).astype(jnp.int32)
    slot_owner = jnp.arange(OWNERS * MAXB, dtype=jnp.int32) // MAXB
    slot_within = jnp.arange(OWNERS * MAXB, dtype=jnp.int32) % MAXB
    valid = slot_within < counts[slot_owner]
    source = jnp.clip(starts[slot_owner] + slot_within, 0, BLOCKS - 1).astype(jnp.int32)
    return (gather_index, source, valid)

def reference(hidden_in, norm_gain, normed_grad, key_grad, weight_blocks, block_count):
    group_rows = D // QUARTERS
    pieces = []
    layouts = []
    for group in range(QUARTERS):
        gather_index, source, valid = block_layout(block_count[group])
        layouts.append((source, valid))
        rows = weight_blocks[:, group].reshape(OWNERS * MAXB, 128)
        pieces.append(rows[gather_index].reshape(group_rows, KVW))
    weight = jnp.concatenate(pieces, axis=0)
    gain = norm_gain.astype(jnp.float32)

    def step(total, items):
        hblock, nblock, kblock = items
        hfloat = hblock.astype(jnp.float32)
        rstd = lax.rsqrt(lax.optimization_barrier(jnp.sum(hfloat * hfloat, axis=1)) / D + EPS)
        normed = (hfloat * rstd[:, None] * gain).astype(jnp.bfloat16)
        total = total + lax.dot_general(normed, kblock, (((0,), (0,)), ((), ())), preferred_element_type=jnp.float32)
        dnorm = nblock.astype(jnp.float32) + lax.dot_general(kblock, weight, (((1,), (1,)), ((), ())), preferred_element_type=jnp.float32)
        proj = lax.optimization_barrier(jnp.sum(gain * dnorm * hfloat, axis=1))
        grad = gain * dnorm * rstd[:, None] - hfloat * (rstd ** 3 * proj / D)[:, None]
        return (total, grad.astype(jnp.bfloat16))
    hsplit = hidden_in.reshape(OWNERS, TOK_DEV, D)
    nsplit = normed_grad.reshape(OWNERS, TOK_DEV, D)
    ksplit = key_grad.reshape(OWNERS, TOK_DEV, KVW)
    dweight, grads = lax.scan(step, jnp.zeros((D, KVW), jnp.float32), (hsplit, nsplit, ksplit))
    outs = []
    for group in range(QUARTERS):
        source, valid = layouts[group]
        flat = dweight[group * group_rows:(group + 1) * group_rows].reshape(BLOCKS, 128)
        padded = jnp.where(valid[:, None], flat[source], jnp.float32(0.0))
        outs.append(padded.reshape(OWNERS, MAXB, 128))
    weight_grad = jnp.stack(outs, axis=1)
    return (grads.reshape(TOKENS, D), weight_grad)
```

```python
import jax
import jax.numpy as jnp
from jax import lax
from jax.experimental import pallas as pl
from jax.experimental.pallas import tpu as pltpu
from jax.sharding import PartitionSpec as P

EPS = 1e-06
LANES = 128


def ceil_to(n, m):
    return (n + m - 1) // m * m


def power_of_two(n):
    return n & (n - 1) == 0


def relative(n, r):
    if power_of_two(n):
        return [(i, i ^ r) for i in range(n)]
    return [(i, (i + r) % n) for i in range(n)]


def relative_index(n, me, r):
    if power_of_two(n):
        return me ^ r
    return lax.rem(me + (n - r), n)


def gather_relatives(x, axis, n):
    known = {0: x}
    if power_of_two(n):
        basis = n - 1
        while basis:
            for r in list(known):
                known[r ^ basis] = lax.ppermute(known[r], axis, relative(n, basis))
            basis //= 2
    else:
        for r in range(1, n):
            known[r] = lax.ppermute(x, axis, relative(n, r))
    return known


def axis_sum(x, axis, n):
    if power_of_two(n):
        bit = 1
        while bit < n:
            x = x + lax.ppermute(x, axis, relative(n, bit))
            bit *= 2
        return x
    return lax.psum(x, axis)


def input_grad_kernel(owner_of, most, counts, place, key, grad, hidden, gain, *refs):
    pieces, (scaled, proj, dense, starts) = refs[:-4], refs[-4:]
    owners = counts.shape[0]

    def mark(o, at):
        starts[o] = at
        return at + counts[o]

    lax.fori_loop(0, owners, mark, jnp.int32(0))
    slot = lax.broadcasted_iota(jnp.int32, (most, LANES), 0)
    index = 0
    for piece in pieces:
        for i in range(piece.shape[0]):
            owner = owner_of(place[0], place[1], index)
            rows = pl.ds(starts[owner], most)
            new = piece[i].astype(jnp.float32)
            dense[rows, :] = jnp.where(slot < counts[owner], new, dense[rows, :])
            index += 1
    tokens, features = hidden.shape
    parts = key.shape[1] // LANES
    step = 256 if features % 256 == 0 else features
    total = jnp.zeros((tokens, LANES), jnp.float32)
    for at in range(0, features, step):
        weight = jnp.concatenate(
            [dense[pl.ds(at * parts + c, step, stride=parts), :] for c in range(parts)], axis=1
        ).astype(jnp.bfloat16)
        cols = slice(at, at + step)
        product = lax.dot_general(
            key[...], weight, (((1,), (1,)), ((), ())), preferred_element_type=jnp.float32
        )
        gained = gain[:, cols] * (grad[:, cols].astype(jnp.float32) + product)
        scaled[:, cols] = gained
        terms = gained * hidden[:, cols].astype(jnp.float32)
        for c in range(0, step, LANES):
            total = total + terms[:, c : c + LANES]
    proj[...] = jnp.sum(total, axis=1, keepdims=True)


def weight_grad_kernel(inner, group_blocks, most, counts, place, *refs):
    norms, keys = refs[: (len(refs) - 3) // 2], refs[(len(refs) - 3) // 2 : -3]
    sent, kept, flat = refs[-3:]
    rows = norms[0].shape[1]
    parts = keys[0].shape[1] // LANES
    step = 256 if rows % 256 == 0 else rows
    for at in range(0, rows, step):
        total = None
        for norm, key in zip(norms, keys):
            part = lax.dot_general(
                norm[:, at : at + step],
                key[...],
                (((0,), (0,)), ((), ())),
                preferred_element_type=jnp.float32,
            )
            total = part if total is None else total + part
        for c in range(parts):
            flat[pl.ds(at * parts + c, step, stride=parts), :] = total[:, c * LANES : (c + 1) * LANES]
    outer_index, inner_index = place[0], place[1]
    lead = lax.rem(outer_index * group_blocks, parts)
    for k in range(inner):
        owner = inner_index ^ k

        def add(j, at):
            return at + jnp.where(j < owner, counts[outer_index * inner + j], 0)

        start = lax.fori_loop(0, inner, add, lead)
        target = sent if k % 2 else kept
        target[k // 2] = flat[pl.ds(start, most), :]


def shards(hidden_in, norm_gain, normed_grad, key_grad, weight_blocks, block_count):
    outer, inner, halves = lax.axis_size("gx"), lax.axis_size("gy"), lax.axis_size("gz")
    owners = outer * inner
    most = weight_blocks.shape[2]
    tokens, features = hidden_in.shape
    width = key_grad.shape[1]
    parts = width // LANES
    blocks = features * parts
    group_blocks = (blocks + outer - 1) // outer
    model_width = features * halves
    gx, gy = lax.axis_index("gx"), lax.axis_index("gy")
    counts = block_count[0]
    place = jnp.stack([gx, gy]).astype(jnp.int32)

    found = gather_relatives(weight_blocks.reshape(most, LANES), "gx", outer)
    order = list(found)
    column = jnp.stack([found[r] for r in order])
    spread = {0: column}
    bit = inner // 2
    while bit:
        for r in list(spread):
            spread[r ^ bit] = lax.ppermute(spread[r], "gy", relative(inner, bit))
        bit //= 2
    names = [(r, s) for s in spread for r in order]

    def owner_of(i, j, index):
        r, s = names[index]
        return relative_index(outer, i, r) * inner + (j ^ s)

    hfloat = hidden_in.astype(jnp.float32)
    squares = axis_sum(jnp.sum(hfloat * hfloat, axis=1), "gz", halves)
    rstd = lax.rsqrt(squares / model_width + EPS)
    normed = (hfloat * rstd[:, None] * norm_gain).astype(jnp.bfloat16)

    rows = max(
        ((i + 1) * group_blocks + parts - 1) // parts - i * group_blocks // parts
        for i in range(outer)
    )
    reach = (outer - 1) * group_blocks // parts + rows
    padded = jnp.pad(normed, ((0, 0), (0, max(0, reach - features))))

    def window(member):
        return lax.dynamic_slice(padded, (0, member * group_blocks // parts), (tokens, rows))

    keys = gather_relatives(key_grad, "gx", outer)
    norms = {0: window(gx)}
    for r in range(1, outer):
        target = gx ^ r if power_of_two(outer) else lax.rem(gx + r, outer)
        norms[r] = lax.ppermute(window(target), "gx", relative(outer, r))

    smem = pl.BlockSpec(memory_space=pltpu.SMEM)
    vmem = pl.BlockSpec(memory_space=pltpu.VMEM)
    pieces = [spread[s] for s in spread]
    scaled, proj = pl.pallas_call(
        lambda *refs: input_grad_kernel(owner_of, most, *refs),
        name="input_grad",
        out_shape=(
            jax.ShapeDtypeStruct((tokens, features), jnp.float32),
            jax.ShapeDtypeStruct((tokens, 1), jnp.float32),
        ),
        in_specs=[smem, smem] + [vmem] * (4 + len(pieces)),
        out_specs=(vmem, vmem),
        scratch_shapes=[
            pltpu.VMEM((ceil_to(blocks + most, 8), LANES), jnp.float32),
            pltpu.SMEM((owners,), jnp.int32),
        ],
    )(counts, place, key_grad, normed_grad, hidden_in, norm_gain[None, :], *pieces)
    proj = axis_sum(proj[:, 0], "gz", halves)
    grad = scaled * rstd[:, None] - hfloat * (rstd**3 * proj / model_width)[:, None]
    hidden_grad = grad.astype(jnp.bfloat16)

    half = jax.ShapeDtypeStruct((inner // 2, most, LANES), jnp.float32)
    sent, kept = pl.pallas_call(
        lambda *refs: weight_grad_kernel(inner, group_blocks, most, *refs),
        name="weight_grad",
        out_shape=(half, half),
        in_specs=[smem, smem] + [vmem] * (2 * outer),
        out_specs=(vmem, vmem),
        scratch_shapes=[pltpu.VMEM((ceil_to(rows * parts + most, 8), LANES), jnp.float32)],
    )(counts, place, *[norms[r] for r in range(outer)], *[keys[r] for r in range(outer)])
    bit = 1
    while True:
        got = lax.ppermute(sent, "gy", relative(inner, bit))
        bit *= 2
        if bit == inner:
            break
        sent, kept = kept[1::2] + got[1::2], kept[0::2] + got[0::2]
    owned = (kept + got)[0]
    count = lax.dynamic_index_in_dim(counts, gx * inner + gy, 0, keepdims=False)
    slots = lax.broadcasted_iota(jnp.int32, (most, LANES), 0)
    owned = jnp.where(slots < count, owned, jnp.float32(0.0))
    return (hidden_grad, owned.reshape(1, 1, most, LANES))


def solution(mesh):
    placed = (
        P(("gx", "gy"), "gz"),
        P("gz"),
        P(("gx", "gy"), "gz"),
        P(("gx", "gy"), None),
        P(("gx", "gy"), "gz", None, None),
        P("gz", None),
    )
    return jax.shard_map(
        shards,
        mesh=mesh,
        in_specs=placed,
        out_specs=(P(("gx", "gy"), "gz"), P(("gx", "gy"), "gz", None, None)),
        check_vma=False,
    )
```

```python
import functools

import jax
import jax.numpy as jnp
from jax import lax
from jax.experimental import pallas as pl
from jax.experimental.pallas import tpu as pltpu
from jax.sharding import PartitionSpec as P

EPS = 1e-06
LANES = 128


def ceil_to(n, m):
    return (n + m - 1) // m * m


def power_of_two(n):
    return n & (n - 1) == 0


def relative(n, r):
    if power_of_two(n):
        return [(i, i ^ r) for i in range(n)]
    return [(i, (i + r) % n) for i in range(n)]


def relative_index(n, me, r):
    if power_of_two(n):
        return me ^ r
    return lax.rem(me + (n - r), n)


def gather_relatives(x, axis, n):
    known = {0: x}
    if power_of_two(n):
        basis = n - 1
        while basis:
            for r in list(known):
                known[r ^ basis] = lax.ppermute(known[r], axis, relative(n, basis))
            basis //= 2
    else:
        for r in range(1, n):
            known[r] = lax.ppermute(x, axis, relative(n, r))
    return known


def axis_terms(x, axis, n):
    if not power_of_two(n):
        return lax.psum(x, axis), jnp.zeros_like(x)
    bit = 1
    while True:
        got = lax.ppermute(x, axis, relative(n, bit)) if n > 1 else jnp.zeros_like(x)
        bit *= 2
        if bit >= n:
            return x, got
        x = x + got


def column(row, lanes):
    return jnp.transpose(jnp.broadcast_to(row, (lanes, row.shape[1])))


def norm_kernel(members, model_width, starts, rows, place, square, other, hidden, gain, *outs):
    tokens, features = hidden.shape
    total = square[...] + other[...]
    rstd = column(lax.rsqrt(total / model_width + EPS), LANES)

    def scale(cols):
        return (hidden[:, cols].astype(jnp.float32) * rstd[:, :1]) * gain[:, cols]

    aligned = rows % LANES == 0 and all(s == i * rows for i, s in enumerate(starts))
    for r, out in enumerate(outs):
        member = members(place[0], r)
        if aligned:
            for at in range(0, rows, LANES):
                cols = pl.ds(pl.multiple_of(member * rows + at, LANES), LANES)
                part = (hidden[:, cols].astype(jnp.float32) * rstd) * gain[:, cols]
                out[:, at : at + LANES] = part.astype(jnp.bfloat16)
        else:
            for i, start in enumerate(starts):

                @pl.when(member == i)
                def _(out=out, start=start):
                    end = min(features, start + rows)
                    part = scale(slice(start, end))
                    if end - start < rows:
                        fill = jnp.zeros((tokens, rows - (end - start)), jnp.float32)
                        part = jnp.concatenate([part, fill], axis=1)
                    out[...] = part.astype(jnp.bfloat16)


def finish_kernel(model_width, square, other, proj, proj_other, scaled, hidden, out):
    rstd = lax.rsqrt((square[...] + other[...]) / model_width + EPS)
    shift = rstd**3 * (proj[...] + proj_other[...]) / model_width
    rstd, shift = column(rstd, LANES), column(shift, LANES)
    for at in range(0, hidden.shape[1], LANES):
        cols = slice(at, at + LANES)
        grad = scaled[:, cols] * rstd - hidden[:, cols].astype(jnp.float32) * shift
        out[:, cols] = grad.astype(jnp.bfloat16)


def input_grad_kernel(owner_of, most, counts, place, key, grad, hidden, gain, *refs):
    pieces, (scaled, proj, dense, starts) = refs[:-4], refs[-4:]
    owners = counts.shape[0]

    def mark(o, at):
        starts[o] = at
        return at + counts[o]

    lax.fori_loop(0, owners, mark, jnp.int32(0))
    slot = lax.broadcasted_iota(jnp.int32, (most, LANES), 0)
    index = 0
    for piece in pieces:
        for i in range(piece.shape[0]):
            owner = owner_of(place[0], place[1], index)
            rows = pl.ds(starts[owner], most)
            new = piece[i].astype(jnp.float32)
            dense[rows, :] = jnp.where(slot < counts[owner], new, dense[rows, :])
            index += 1
    tokens, features = hidden.shape
    parts = key.shape[1] // LANES
    step = 256 if features % 256 == 0 else features
    total = jnp.zeros((tokens, LANES), jnp.float32)
    for at in range(0, features, step):
        weight = jnp.concatenate(
            [dense[pl.ds(at * parts + c, step, stride=parts), :] for c in range(parts)], axis=1
        ).astype(jnp.bfloat16)
        cols = slice(at, at + step)
        product = lax.dot_general(
            key[...], weight, (((1,), (1,)), ((), ())), preferred_element_type=jnp.float32
        )
        gained = gain[:, cols] * (grad[:, cols].astype(jnp.float32) + product)
        scaled[:, cols] = gained
        terms = gained * hidden[:, cols].astype(jnp.float32)
        for c in range(0, step, LANES):
            total = total + terms[:, c : c + LANES]
    proj[...] = jnp.sum(jnp.transpose(total), axis=0, keepdims=True)


def weight_grad_kernel(inner, group_blocks, most, counts, place, *refs):
    norms, keys = refs[: (len(refs) - 3) // 2], refs[(len(refs) - 3) // 2 : -3]
    sent, kept, flat = refs[-3:]
    rows = norms[0].shape[1]
    parts = keys[0].shape[1] // LANES
    step = 256 if rows % 256 == 0 else rows
    for at in range(0, rows, step):
        total = None
        for norm, key in zip(norms, keys):
            part = lax.dot_general(
                norm[:, at : at + step],
                key[...],
                (((0,), (0,)), ((), ())),
                preferred_element_type=jnp.float32,
            )
            total = part if total is None else total + part
        for c in range(parts):
            flat[pl.ds(at * parts + c, step, stride=parts), :] = total[:, c * LANES : (c + 1) * LANES]
    outer_index, inner_index = place[0], place[1]
    lead = lax.rem(outer_index * group_blocks, parts)
    for k in range(inner):
        owner = inner_index ^ k

        def add(j, at):
            return at + jnp.where(j < owner, counts[outer_index * inner + j], 0)

        start = lax.fori_loop(0, inner, add, lead)
        target = sent if k % 2 else kept
        target[k // 2] = flat[pl.ds(start, most), :]


def shards(hidden_in, norm_gain, normed_grad, key_grad, weight_blocks, block_count):
    outer, inner, halves = lax.axis_size("gx"), lax.axis_size("gy"), lax.axis_size("gz")
    owners = outer * inner
    most = weight_blocks.shape[2]
    tokens, features = hidden_in.shape
    width = key_grad.shape[1]
    parts = width // LANES
    blocks = features * parts
    group_blocks = (blocks + outer - 1) // outer
    model_width = features * halves
    gx, gy = lax.axis_index("gx"), lax.axis_index("gy")
    counts = block_count[0]
    place = jnp.stack([gx, gy]).astype(jnp.int32)

    smem = pl.BlockSpec(memory_space=pltpu.SMEM)
    vmem = pl.BlockSpec(memory_space=pltpu.VMEM)

    def call(kernel, out_shape, scalars, arrays, scratch=(), megabytes=16):
        single = not isinstance(out_shape, tuple)
        return pl.pallas_call(
            kernel,
            out_shape=out_shape,
            in_specs=[smem] * len(scalars) + [vmem] * len(arrays),
            out_specs=vmem if single else (vmem,) * len(out_shape),
            scratch_shapes=list(scratch),
            compiler_params=pltpu.CompilerParams(vmem_limit_bytes=megabytes << 20),
        )(*scalars, *arrays)

    found = gather_relatives(weight_blocks.reshape(most, LANES), "gx", outer)
    order = list(found)
    lots = [order[: len(order) // 2], order[len(order) // 2 :]]
    pieces, names = [], []
    for lot in lots:
        spread = {0: jnp.stack([found[r] for r in lot])}
        bit = inner // 2
        while bit:
            for r in list(spread):
                spread[r ^ bit] = lax.ppermute(spread[r], "gy", relative(inner, bit))
            bit //= 2
        pieces += list(spread.values())
        names += [(r, s) for s in spread for r in lot]

    def owner_of(i, j, index):
        r, s = names[index]
        return relative_index(outer, i, r) * inner + (j ^ s)

    hfloat = hidden_in.astype(jnp.float32)
    square = jnp.sum(hfloat * hfloat, axis=1)
    squares = [t[None, :] for t in axis_terms(square, "gz", halves)]
    gain = norm_gain[None, :]

    starts = [i * group_blocks // parts for i in range(outer)]
    rows = max(
        ((i + 1) * group_blocks + parts - 1) // parts - starts[i] for i in range(outer)
    )

    def target(i, r):
        return i ^ r if power_of_two(outer) else lax.rem(i + r, outer)

    window = jax.ShapeDtypeStruct((tokens, rows), jnp.bfloat16)
    windows = call(
        functools.partial(norm_kernel, target, model_width, starts, rows),
        (window,) * outer,
        [place],
        [*squares, hidden_in, gain],
    )
    keys = gather_relatives(key_grad, "gx", outer)
    norms = [windows[0]]
    for r in range(1, outer):
        norms.append(lax.ppermute(windows[r], "gx", relative(outer, r)))

    scaled, proj = call(
        functools.partial(input_grad_kernel, owner_of, most),
        (
            jax.ShapeDtypeStruct((tokens, features), jnp.float32),
            jax.ShapeDtypeStruct((1, tokens), jnp.float32),
        ),
        [counts, place],
        [key_grad, normed_grad, hidden_in, gain, *pieces],
        [
            pltpu.VMEM((ceil_to(blocks + most, 8), LANES), jnp.float32),
            pltpu.SMEM((owners,), jnp.int32),
        ],
    )
    projs = axis_terms(proj, "gz", halves)
    hidden_grad = call(
        functools.partial(finish_kernel, model_width),
        jax.ShapeDtypeStruct((tokens, features), jnp.bfloat16),
        [],
        [*squares, *projs, scaled, hidden_in],
    )

    half = jax.ShapeDtypeStruct((inner // 2, most, LANES), jnp.float32)
    sent, kept = call(
        functools.partial(weight_grad_kernel, inner, group_blocks, most),
        (half, half),
        [counts, place],
        [*norms, *[keys[r] for r in range(outer)]],
        [pltpu.VMEM((ceil_to(rows * parts + most, 8), LANES), jnp.float32)],
    )
    bit = 1
    while True:
        got = lax.ppermute(sent, "gy", relative(inner, bit))
        bit *= 2
        if bit == inner:
            break
        sent, kept = kept[1::2] + got[1::2], kept[0::2] + got[0::2]
    owned = (kept + got)[0]
    count = lax.dynamic_index_in_dim(counts, gx * inner + gy, 0, keepdims=False)
    slots = lax.broadcasted_iota(jnp.int32, (most, LANES), 0)
    owned = jnp.where(slots < count, owned, jnp.float32(0.0))
    return (hidden_grad, owned.reshape(1, 1, most, LANES))


def solution(mesh):
    placed = (
        P(("gx", "gy"), "gz"),
        P("gz"),
        P(("gx", "gy"), "gz"),
        P(("gx", "gy"), None),
        P(("gx", "gy"), "gz", None, None),
        P("gz", None),
    )
    return jax.shard_map(
        shards,
        mesh=mesh,
        in_specs=placed,
        out_specs=(P(("gx", "gy"), "gz"), P(("gx", "gy"), "gz", None, None)),
        check_vma=False,
    )
```

```python
import functools

import jax
import jax.numpy as jnp
from jax import lax
from jax.experimental import pallas as pl
from jax.experimental.pallas import tpu as pltpu
from jax.sharding import PartitionSpec as P

EPS = 1e-06
LANES = 128
PLACE = 3


def ceil_to(n, m):
    return (n + m - 1) // m * m


def power_of_two(n):
    return n & (n - 1) == 0


def relative(n, r):
    if power_of_two(n):
        return [(i, i ^ r) for i in range(n)]
    return [(i, (i + r) % n) for i in range(n)]


def relative_index(n, me, r):
    if power_of_two(n):
        return me ^ r
    return lax.rem(me + (n - r), n)


def gather_relatives(x, axis, n):
    known = {0: x}
    if power_of_two(n):
        basis = n - 1
        while basis:
            for r in list(known):
                known[r ^ basis] = lax.ppermute(known[r], axis, relative(n, basis))
            basis //= 2
    else:
        for r in range(1, n):
            known[r] = lax.ppermute(x, axis, relative(n, r))
    return known


def axis_terms(x, axis, n):
    if not power_of_two(n):
        return lax.psum(x, axis), jnp.zeros_like(x)
    bit = 1
    while True:
        got = lax.ppermute(x, axis, relative(n, bit)) if n > 1 else jnp.zeros_like(x)
        bit *= 2
        if bit >= n:
            return x, got
        x = x + got


def column(row, lanes):
    return jnp.transpose(jnp.broadcast_to(row, (lanes, row.shape[1])))


def load_kernel(share, blocks, key, hidden, parcel, square, loaded, sems):
    parts = key.shape[1] // LANES
    at = 0
    if share < key.shape[0]:
        at = pl.multiple_of(lax.axis_index("gz") * share, share)
    pairs = [(hidden, loaded), (blocks, parcel.at[pl.ds(parts * share, blocks.shape[0]), :])]
    for c in range(parts):
        part = key.at[pl.ds(at, share), c * LANES : (c + 1) * LANES]
        pairs.append((part, parcel.at[c * share : (c + 1) * share, :]))
    copies = [pltpu.make_async_copy(a, b, sems.at[i]) for i, (a, b) in enumerate(pairs)]
    for copy in copies:
        copy.start()
    copies[0].wait()
    total = jnp.zeros((hidden.shape[0], LANES), jnp.float32)
    for c in range(0, hidden.shape[1], LANES):
        value = loaded[:, c : c + LANES].astype(jnp.float32)
        total = total + value * value
    square[...] = jnp.sum(jnp.transpose(total), axis=0, keepdims=True)
    for copy in copies[1:]:
        copy.wait()


def norm_kernel(members, model_width, starts, rows, meta, square, other, hidden, gain, *outs):
    tokens, features = hidden.shape
    total = square[...] + other[...]
    rstd = column(lax.rsqrt(total / model_width + EPS), LANES)

    def scale(cols):
        return (hidden[:, cols].astype(jnp.float32) * rstd[:, :1]) * gain[:, cols]

    aligned = rows % LANES == 0 and all(s == i * rows for i, s in enumerate(starts))
    for r, out in enumerate(outs):
        member = members(meta[0], r)
        if aligned:
            for at in range(0, rows, LANES):
                cols = pl.ds(pl.multiple_of(member * rows + at, LANES), LANES)
                part = (hidden[:, cols].astype(jnp.float32) * rstd) * gain[:, cols]
                out[:, at : at + LANES] = part.astype(jnp.bfloat16)
        else:
            for i, start in enumerate(starts):

                @pl.when(member == i)
                def _(out=out, start=start):
                    end = min(features, start + rows)
                    part = scale(slice(start, end))
                    if end - start < rows:
                        fill = jnp.zeros((tokens, rows - (end - start)), jnp.float32)
                        part = jnp.concatenate([part, fill], axis=1)
                    out[...] = part.astype(jnp.bfloat16)


def finish_kernel(model_width, square, other, proj, proj_other, scaled, hidden, out):
    rstd = lax.rsqrt((square[...] + other[...]) / model_width + EPS)
    shift = rstd**3 * (proj[...] + proj_other[...]) / model_width
    rstd, shift = column(rstd, LANES), column(shift, LANES)
    for at in range(0, hidden.shape[1], LANES):
        cols = slice(at, at + LANES)
        grad = scaled[:, cols] * rstd - hidden[:, cols].astype(jnp.float32) * shift
        out[:, cols] = grad.astype(jnp.bfloat16)


def input_grad_kernel(owner_of, most, meta, key, grad, hidden, gain, *refs):
    pieces, (scaled, proj, dense, starts) = refs[:-4], refs[-4:]
    owners = meta.shape[0] - PLACE

    def mark(o, at):
        starts[o] = at
        return at + meta[PLACE + o]

    lax.fori_loop(0, owners, mark, jnp.int32(0))
    slot = lax.broadcasted_iota(jnp.int32, (most, LANES), 0)
    index = 0
    for piece in pieces:
        for i in range(piece.shape[0]):
            owner = owner_of(meta[0], meta[1], index)
            rows = pl.ds(starts[owner], most)
            new = piece[i].astype(jnp.float32)
            dense[rows, :] = jnp.where(slot < meta[PLACE + owner], new, dense[rows, :])
            index += 1
    tokens, features = hidden.shape
    parts = key.shape[1] // LANES
    step = 256 if features % 256 == 0 else features
    total = jnp.zeros((tokens, LANES), jnp.float32)
    for at in range(0, features, step):
        weight = jnp.concatenate(
            [dense[pl.ds(at * parts + c, step, stride=parts), :] for c in range(parts)], axis=1
        ).astype(jnp.bfloat16)
        cols = slice(at, at + step)
        product = lax.dot_general(
            key[...], weight, (((1,), (1,)), ((), ())), preferred_element_type=jnp.float32
        )
        gained = gain[:, cols] * (grad[:, cols].astype(jnp.float32) + product)
        scaled[:, cols] = gained
        terms = gained * hidden[:, cols].astype(jnp.float32)
        for c in range(0, step, LANES):
            total = total + terms[:, c : c + LANES]
    proj[...] = jnp.sum(jnp.transpose(total), axis=0, keepdims=True)


def weight_grad_kernel(sources, inner, group_blocks, most, meta, own, *refs):
    sent, kept, flat, whole = refs[-4:]
    pieces, norms = refs[: len(sources)], refs[len(sources) : -4]
    tokens, width = own.shape
    rows = norms[0].shape[1]
    parts = width // LANES
    whole[:tokens, :] = own[...]
    for (member, lot, share), piece in zip(sources, pieces):
        offset = member(meta[2]) * share
        for i, r in enumerate(lot):
            for c in range(parts):
                target = pl.ds(pl.multiple_of(r * tokens + offset, share), share)
                whole[target, c * LANES : (c + 1) * LANES] = piece[i, c * share : (c + 1) * share, :]
    step = 256 if rows % 256 == 0 else rows
    for at in range(0, rows, step):
        total = None
        for r, norm in enumerate(norms):
            part = lax.dot_general(
                norm[:, at : at + step],
                whole[r * tokens : (r + 1) * tokens, :],
                (((0,), (0,)), ((), ())),
                preferred_element_type=jnp.float32,
            )
            total = part if total is None else total + part
        for c in range(parts):
            flat[pl.ds(at * parts + c, step, stride=parts), :] = total[:, c * LANES : (c + 1) * LANES]
    outer_index, inner_index = meta[0], meta[1]
    slot = lax.broadcasted_iota(jnp.int32, (most, LANES), 0)
    lead = lax.rem(outer_index * group_blocks, parts)
    for k in range(inner):
        owner = inner_index ^ k

        def add(j, at):
            return at + jnp.where(j < owner, meta[PLACE + outer_index * inner + j], 0)

        start = lax.fori_loop(0, inner, add, lead)
        target = sent if k % 2 else kept
        target[k // 2] = jnp.where(
            slot < meta[PLACE + outer_index * inner + owner], flat[pl.ds(start, most), :], 0.0
        )


def shards(hidden_in, norm_gain, normed_grad, key_grad, weight_blocks, block_count):
    outer, inner, halves = lax.axis_size("gx"), lax.axis_size("gy"), lax.axis_size("gz")
    owners = outer * inner
    most = weight_blocks.shape[2]
    tokens, features = hidden_in.shape
    width = key_grad.shape[1]
    parts = width // LANES
    blocks = features * parts
    group_blocks = (blocks + outer - 1) // outer
    model_width = features * halves
    gx, gy, gz = (lax.axis_index(name) for name in ("gx", "gy", "gz"))
    place = jnp.stack([gx, gy, gz]).astype(jnp.int32)
    meta = jnp.concatenate([place, block_count[0]])

    smem = pl.BlockSpec(memory_space=pltpu.SMEM)
    vmem = pl.BlockSpec(memory_space=pltpu.VMEM)

    def call(kernel, out_shape, scalars, arrays, scratch=(), megabytes=4):
        single = not isinstance(out_shape, tuple)
        return pl.pallas_call(
            kernel,
            out_shape=out_shape,
            in_specs=[smem] * len(scalars) + [vmem] * len(arrays),
            out_specs=vmem if single else (vmem,) * len(out_shape),
            scratch_shapes=list(scratch),
            compiler_params=pltpu.CompilerParams(vmem_limit_bytes=megabytes << 20),
        )(*scalars, *arrays)

    share = tokens // halves
    split = halves > 1 and tokens % halves == 0 and share % 16 == 0
    share = share if split else tokens
    head = share * parts
    hbm = pl.BlockSpec(memory_space=pltpu.HBM)
    parcel, square = pl.pallas_call(
        functools.partial(load_kernel, share),
        name="load",
        out_shape=(
            jax.ShapeDtypeStruct((head + most, LANES), jnp.bfloat16),
            jax.ShapeDtypeStruct((1, tokens), jnp.float32),
        ),
        in_specs=[hbm] * 3,
        out_specs=(vmem, vmem),
        scratch_shapes=[
            pltpu.VMEM((tokens, features), jnp.bfloat16),
            pltpu.SemaphoreType.DMA((parts + 2,)),
        ],
        compiler_params=pltpu.CompilerParams(vmem_limit_bytes=60 << 20),
    )(weight_blocks.reshape(most, LANES), key_grad, hidden_in)
    hidden, gain = hidden_in, norm_gain[None, :]
    found = gather_relatives(parcel, "gx", outer)
    order = list(found)
    lots = [lot for lot in (order[:1], order[1:-1], order[-1:]) if lot]
    lots = lots if outer > 1 else [order]

    pieces, names = [], []
    for lot_index, lot in enumerate(lots):
        own = weight_blocks.reshape(1, most, LANES)
        spread = {0: jnp.stack([found[r][head:] for r in lot]) if lot_index else own}
        bit = inner // 2
        while bit:
            for r in list(spread):
                spread[r ^ bit] = lax.ppermute(spread[r], "gy", relative(inner, bit))
            bit //= 2
        pieces += list(spread.values())
        names += [(r, s) for s in spread for r in lot]

    def owner_of(i, j, index):
        r, s = names[index]
        return relative_index(outer, i, r) * inner + (j ^ s)

    squares = axis_terms(square, "gz", halves)

    starts = [i * group_blocks // parts for i in range(outer)]
    rows = max(
        ((i + 1) * group_blocks + parts - 1) // parts - starts[i] for i in range(outer)
    )

    def target(i, r):
        return i ^ r if power_of_two(outer) else lax.rem(i + r, outer)

    window = jax.ShapeDtypeStruct((tokens, rows), jnp.bfloat16)
    windows = call(
        functools.partial(norm_kernel, target, model_width, starts, rows),
        (window,) * outer,
        [meta],
        [*squares, hidden, gain],
    )

    sources, key_pieces = [], []
    for r in order[1:]:
        member = functools.partial(relative_index, halves, r=0) if split else (lambda i: 0)
        sources.append((member, [r], share))
        key_pieces.append(found[r][None])
    for lot in [order[1:-1], order[-1:]] if split and outer > 1 else []:
        stack = jnp.stack([found[r][:head] for r in lot])
        for s in range(1, halves):
            sources.append((functools.partial(relative_index, halves, r=s), lot, share))
            key_pieces.append(lax.ppermute(stack, "gz", relative(halves, s)))
    norms = [windows[0]]
    for r in range(1, outer):
        norms.append(lax.ppermute(windows[r], "gx", relative(outer, r)))

    scaled, proj = call(
        functools.partial(input_grad_kernel, owner_of, most),
        (
            jax.ShapeDtypeStruct((tokens, features), jnp.float32),
            jax.ShapeDtypeStruct((1, tokens), jnp.float32),
        ),
        [meta],
        [key_grad, normed_grad, hidden, gain, *pieces],
        [
            pltpu.VMEM((ceil_to(blocks + most, 8), LANES), jnp.float32),
            pltpu.SMEM((owners,), jnp.int32),
        ],
        megabytes=8,
    )
    projs = axis_terms(proj, "gz", halves)
    hidden_grad = call(
        functools.partial(finish_kernel, model_width),
        jax.ShapeDtypeStruct((tokens, features), jnp.bfloat16),
        [],
        [*squares, *projs, scaled, hidden],
    )

    half = jax.ShapeDtypeStruct((inner // 2, most, LANES), jnp.float32)
    sent, kept = call(
        functools.partial(weight_grad_kernel, sources, inner, group_blocks, most),
        (half, half),
        [meta],
        [key_grad, *key_pieces, *norms],
        [
            pltpu.VMEM((ceil_to(rows * parts + most, 8), LANES), jnp.float32),
            pltpu.VMEM((outer * tokens, width), jnp.bfloat16),
        ],
    )
    bit = 1
    while True:
        got = lax.ppermute(sent, "gy", relative(inner, bit))
        bit *= 2
        if bit == inner:
            break
        sent, kept = kept[1::2] + got[1::2], kept[0::2] + got[0::2]
    owned = (kept + got)[0]
    return (hidden_grad, owned.reshape(1, 1, most, LANES))


def solution(mesh):
    placed = (
        P(("gx", "gy"), "gz"),
        P("gz"),
        P(("gx", "gy"), "gz"),
        P(("gx", "gy"), None),
        P(("gx", "gy"), "gz", None, None),
        P("gz", None),
    )
    return jax.shard_map(
        shards,
        mesh=mesh,
        in_specs=placed,
        out_specs=(P(("gx", "gy"), "gz"), P(("gx", "gy"), "gz", None, None)),
        check_vma=False,
    )
```

```python
import functools

import jax
import jax.numpy as jnp
from jax import lax
from jax.experimental import pallas as pl
from jax.experimental.pallas import tpu as pltpu
from jax.sharding import PartitionSpec as P

EPS = 1e-06
LANES = 128
PLACE = 3


def ceil_to(n, m):
    return (n + m - 1) // m * m


def power_of_two(n):
    return n & (n - 1) == 0


def relative(n, r):
    if power_of_two(n):
        return [(i, i ^ r) for i in range(n)]
    return [(i, (i + r) % n) for i in range(n)]


def relative_index(n, me, r):
    if power_of_two(n):
        return me ^ r
    return lax.rem(me + (n - r), n)


def gather_relatives(blocks, part, parcel, axis, n):
    head = part.shape[0]
    found, parts = {0: blocks}, {0: part}

    def both(r):
        parts[r] = lax.ppermute(parcel, axis, relative(n, r))
        found[r] = parts[r][head:]

    if not power_of_two(n):
        for r in range(1, n):
            both(r)
        return found, parts
    basis = n - 1
    while basis:
        for r in list(found):
            if basis == 1 and r == 0:
                both(1)
                continue
            found[r ^ basis] = lax.ppermute(found[r], axis, relative(n, basis))
            parts[r ^ basis] = lax.ppermute(parts[r], axis, relative(n, basis))
        basis //= 2
    return found, parts


def axis_terms(x, axis, n):
    if not power_of_two(n):
        return lax.psum(x, axis), jnp.zeros_like(x)
    bit = 1
    while True:
        got = lax.ppermute(x, axis, relative(n, bit)) if n > 1 else jnp.zeros_like(x)
        bit *= 2
        if bit >= n:
            return x, got
        x = x + got


def column(row, lanes):
    return jnp.transpose(jnp.broadcast_to(row, (lanes, row.shape[1])))


def load_kernel(share, blocks, key, hidden, parcel, own, square, loaded, sems):
    parts = key.shape[1] // LANES
    at = 0
    if share < key.shape[0]:
        at = pl.multiple_of(lax.axis_index("gz") * share, share)
    pairs = [(hidden, loaded), (blocks, parcel.at[pl.ds(parts * share, blocks.shape[0]), :])]
    for c in range(parts):
        part = key.at[pl.ds(at, share), c * LANES : (c + 1) * LANES]
        pairs.append((part, parcel.at[c * share : (c + 1) * share, :]))
        pairs.append((part, own.at[c * share : (c + 1) * share, :]))
    copies = [pltpu.make_async_copy(a, b, sems.at[i]) for i, (a, b) in enumerate(pairs)]
    for copy in copies:
        copy.start()
    copies[0].wait()
    total = jnp.zeros((hidden.shape[0], LANES), jnp.float32)
    for c in range(0, hidden.shape[1], LANES):
        value = loaded[:, c : c + LANES].astype(jnp.float32)
        total = total + value * value
    square[...] = jnp.sum(jnp.transpose(total), axis=0, keepdims=True)
    for copy in copies[1:]:
        copy.wait()


def norm_kernel(members, model_width, starts, rows, meta, square, other, hidden, gain, *outs):
    tokens, features = hidden.shape
    total = square[...] + other[...]
    rstd = column(lax.rsqrt(total / model_width + EPS), LANES)

    def scale(cols):
        return (hidden[:, cols].astype(jnp.float32) * rstd[:, :1]) * gain[:, cols]

    aligned = rows % LANES == 0 and all(s == i * rows for i, s in enumerate(starts))
    for r, out in enumerate(outs):
        member = members(meta[0], r)
        if aligned:
            for at in range(0, rows, LANES):
                cols = pl.ds(pl.multiple_of(member * rows + at, LANES), LANES)
                part = (hidden[:, cols].astype(jnp.float32) * rstd) * gain[:, cols]
                out[:, at : at + LANES] = part.astype(jnp.bfloat16)
        else:
            for i, start in enumerate(starts):

                @pl.when(member == i)
                def _(out=out, start=start):
                    end = min(features, start + rows)
                    part = scale(slice(start, end))
                    if end - start < rows:
                        fill = jnp.zeros((tokens, rows - (end - start)), jnp.float32)
                        part = jnp.concatenate([part, fill], axis=1)
                    out[...] = part.astype(jnp.bfloat16)


def finish_kernel(model_width, square, other, proj, proj_other, scaled, hidden, out):
    rstd = lax.rsqrt((square[...] + other[...]) / model_width + EPS)
    shift = rstd**3 * (proj[...] + proj_other[...]) / model_width
    rstd, shift = column(rstd, LANES), column(shift, LANES)
    for at in range(0, hidden.shape[1], LANES):
        cols = slice(at, at + LANES)
        grad = scaled[:, cols] * rstd - hidden[:, cols].astype(jnp.float32) * shift
        out[:, cols] = grad.astype(jnp.bfloat16)


def input_grad_kernel(owner_of, most, meta, key, grad, hidden, gain, *refs):
    pieces, (scaled, proj, dense, starts) = refs[:-4], refs[-4:]
    owners = meta.shape[0] - PLACE

    def mark(o, at):
        starts[o] = at
        return at + meta[PLACE + o]

    lax.fori_loop(0, owners, mark, jnp.int32(0))
    slot = lax.broadcasted_iota(jnp.int32, (most, LANES), 0)
    index = 0
    for piece in pieces:
        for i in range(piece.shape[0]):
            owner = owner_of(meta[0], meta[1], index)
            rows = pl.ds(starts[owner], most)
            new = piece[i].astype(jnp.float32)
            dense[rows, :] = jnp.where(slot < meta[PLACE + owner], new, dense[rows, :])
            index += 1
    tokens, features = hidden.shape
    parts = key.shape[1] // LANES
    step = 256 if features % 256 == 0 else features
    total = jnp.zeros((tokens, LANES), jnp.float32)
    for at in range(0, features, step):
        weight = jnp.concatenate(
            [dense[pl.ds(at * parts + c, step, stride=parts), :] for c in range(parts)], axis=1
        ).astype(jnp.bfloat16)
        cols = slice(at, at + step)
        product = lax.dot_general(
            key[...], weight, (((1,), (1,)), ((), ())), preferred_element_type=jnp.float32
        )
        gained = gain[:, cols] * (grad[:, cols].astype(jnp.float32) + product)
        scaled[:, cols] = gained
        terms = gained * hidden[:, cols].astype(jnp.float32)
        for c in range(0, step, LANES):
            total = total + terms[:, c : c + LANES]
    proj[...] = jnp.sum(jnp.transpose(total), axis=0, keepdims=True)


def weight_grad_kernel(sources, inner, group_blocks, most, meta, own, *refs):
    sent, kept, flat, whole = refs[-4:]
    pieces, norms = refs[: len(sources)], refs[len(sources) : -4]
    tokens, width = own.shape
    rows = norms[0].shape[1]
    parts = width // LANES
    whole[:tokens, :] = own[...]
    for (member, lot, share), piece in zip(sources, pieces):
        offset = member(meta[2]) * share
        for i, r in enumerate(lot):
            for c in range(parts):
                target = pl.ds(pl.multiple_of(r * tokens + offset, share), share)
                whole[target, c * LANES : (c + 1) * LANES] = piece[i, c * share : (c + 1) * share, :]
    step = 256 if rows % 256 == 0 else rows
    for at in range(0, rows, step):
        total = None
        for r, norm in enumerate(norms):
            part = lax.dot_general(
                norm[:, at : at + step],
                whole[r * tokens : (r + 1) * tokens, :],
                (((0,), (0,)), ((), ())),
                preferred_element_type=jnp.float32,
            )
            total = part if total is None else total + part
        for c in range(parts):
            flat[pl.ds(at * parts + c, step, stride=parts), :] = total[:, c * LANES : (c + 1) * LANES]
    outer_index, inner_index = meta[0], meta[1]
    slot = lax.broadcasted_iota(jnp.int32, (most, LANES), 0)
    lead = lax.rem(outer_index * group_blocks, parts)
    for k in range(inner):
        owner = inner_index ^ k

        def add(j, at):
            return at + jnp.where(j < owner, meta[PLACE + outer_index * inner + j], 0)

        start = lax.fori_loop(0, inner, add, lead)
        target = sent if k % 2 else kept
        target[k // 2] = jnp.where(
            slot < meta[PLACE + outer_index * inner + owner], flat[pl.ds(start, most), :], 0.0
        )


def shards(hidden_in, norm_gain, normed_grad, key_grad, weight_blocks, block_count):
    outer, inner, halves = lax.axis_size("gx"), lax.axis_size("gy"), lax.axis_size("gz")
    owners = outer * inner
    most = weight_blocks.shape[2]
    tokens, features = hidden_in.shape
    width = key_grad.shape[1]
    parts = width // LANES
    blocks = features * parts
    group_blocks = (blocks + outer - 1) // outer
    model_width = features * halves
    gx, gy, gz = (lax.axis_index(name) for name in ("gx", "gy", "gz"))
    place = jnp.stack([gx, gy, gz]).astype(jnp.int32)
    meta = jnp.concatenate([place, block_count[0]])

    smem = pl.BlockSpec(memory_space=pltpu.SMEM)
    vmem = pl.BlockSpec(memory_space=pltpu.VMEM)

    def call(kernel, out_shape, scalars, arrays, scratch=(), megabytes=4):
        single = not isinstance(out_shape, tuple)
        return pl.pallas_call(
            kernel,
            out_shape=out_shape,
            in_specs=[smem] * len(scalars) + [vmem] * len(arrays),
            out_specs=vmem if single else (vmem,) * len(out_shape),
            scratch_shapes=list(scratch),
            compiler_params=pltpu.CompilerParams(vmem_limit_bytes=megabytes << 20),
        )(*scalars, *arrays)

    share = tokens // halves
    split = halves > 1 and tokens % halves == 0 and share % 16 == 0
    share = share if split else tokens
    head = share * parts
    hbm = pl.BlockSpec(memory_space=pltpu.HBM)
    parcel, part, square = pl.pallas_call(
        functools.partial(load_kernel, share),
        name="load",
        out_shape=(
            jax.ShapeDtypeStruct((head + most, LANES), jnp.bfloat16),
            jax.ShapeDtypeStruct((head, LANES), jnp.bfloat16),
            jax.ShapeDtypeStruct((1, tokens), jnp.float32),
        ),
        in_specs=[hbm] * 3,
        out_specs=(vmem, vmem, vmem),
        scratch_shapes=[
            pltpu.VMEM((tokens, features), jnp.bfloat16),
            pltpu.SemaphoreType.DMA((2 * parts + 2,)),
        ],
        compiler_params=pltpu.CompilerParams(vmem_limit_bytes=60 << 20),
    )(weight_blocks.reshape(most, LANES), key_grad, hidden_in)
    hidden, gain = hidden_in, norm_gain[None, :]
    own_blocks = weight_blocks.reshape(most, LANES)
    found, key_parts = gather_relatives(own_blocks, part, parcel, "gx", outer)
    order = list(found)
    lots = [lot for lot in (order[:1], order[1:-1], order[-1:]) if lot]
    lots = lots if outer > 1 else [order]

    pieces, names = [], []
    for lot in lots:
        spread = {0: jnp.stack([found[r] for r in lot])}
        bit = inner // 2
        while bit:
            for r in list(spread):
                spread[r ^ bit] = lax.ppermute(spread[r], "gy", relative(inner, bit))
            bit //= 2
        pieces += list(spread.values())
        names += [(r, s) for s in spread for r in lot]

    def owner_of(i, j, index):
        r, s = names[index]
        return relative_index(outer, i, r) * inner + (j ^ s)

    squares = axis_terms(square, "gz", halves)

    starts = [i * group_blocks // parts for i in range(outer)]
    rows = max(
        ((i + 1) * group_blocks + parts - 1) // parts - starts[i] for i in range(outer)
    )

    def target(i, r):
        return i ^ r if power_of_two(outer) else lax.rem(i + r, outer)

    window = jax.ShapeDtypeStruct((tokens, rows), jnp.bfloat16)
    windows = call(
        functools.partial(norm_kernel, target, model_width, starts, rows),
        (window,) * outer,
        [meta],
        [*squares, hidden, gain],
    )

    sources, key_pieces = [], []
    for r in order[1:]:
        member = functools.partial(relative_index, halves, r=0) if split else (lambda i: 0)
        sources.append((member, [r], share))
        key_pieces.append(key_parts[r][None])
    for lot in [order[1:-1], order[-1:]] if split and outer > 1 else []:
        stack = jnp.stack([key_parts[r][:head] for r in lot])
        for s in range(1, halves):
            sources.append((functools.partial(relative_index, halves, r=s), lot, share))
            key_pieces.append(lax.ppermute(stack, "gz", relative(halves, s)))
    norms = [windows[0]]
    for r in range(1, outer):
        norms.append(lax.ppermute(windows[r], "gx", relative(outer, r)))

    scaled, proj = call(
        functools.partial(input_grad_kernel, owner_of, most),
        (
            jax.ShapeDtypeStruct((tokens, features), jnp.float32),
            jax.ShapeDtypeStruct((1, tokens), jnp.float32),
        ),
        [meta],
        [key_grad, normed_grad, hidden, gain, *pieces],
        [
            pltpu.VMEM((ceil_to(blocks + most, 8), LANES), jnp.float32),
            pltpu.SMEM((owners,), jnp.int32),
        ],
        megabytes=8,
    )
    projs = axis_terms(proj, "gz", halves)
    hidden_grad = call(
        functools.partial(finish_kernel, model_width),
        jax.ShapeDtypeStruct((tokens, features), jnp.bfloat16),
        [],
        [*squares, *projs, scaled, hidden],
    )

    half = jax.ShapeDtypeStruct((inner // 2, most, LANES), jnp.float32)
    sent, kept = call(
        functools.partial(weight_grad_kernel, sources, inner, group_blocks, most),
        (half, half),
        [meta],
        [key_grad, *key_pieces, *norms],
        [
            pltpu.VMEM((ceil_to(rows * parts + most, 8), LANES), jnp.float32),
            pltpu.VMEM((outer * tokens, width), jnp.bfloat16),
        ],
    )
    bit = 1
    while True:
        got = lax.ppermute(sent, "gy", relative(inner, bit))
        bit *= 2
        if bit == inner:
            break
        sent, kept = kept[1::2] + got[1::2], kept[0::2] + got[0::2]
    owned = (kept + got)[0]
    return (hidden_grad, owned.reshape(1, 1, most, LANES))


def solution(mesh):
    placed = (
        P(("gx", "gy"), "gz"),
        P("gz"),
        P(("gx", "gy"), "gz"),
        P(("gx", "gy"), None),
        P(("gx", "gy"), "gz", None, None),
        P("gz", None),
    )
    return jax.shard_map(
        shards,
        mesh=mesh,
        in_specs=placed,
        out_specs=(P(("gx", "gy"), "gz"), P(("gx", "gy"), "gz", None, None)),
        check_vma=False,
    )
```

```python
import functools

import jax
import jax.numpy as jnp
from jax import lax
from jax.experimental import pallas as pl
from jax.experimental.pallas import tpu as pltpu
from jax.sharding import PartitionSpec as P

EPS = 1e-06
LANES = 128
PLACE = 3


def ceil_to(n, m):
    return (n + m - 1) // m * m


def power_of_two(n):
    return n & (n - 1) == 0


def relative(n, r):
    if power_of_two(n):
        return [(i, i ^ r) for i in range(n)]
    return [(i, (i + r) % n) for i in range(n)]


def relative_index(n, me, r):
    if power_of_two(n):
        return me ^ r
    return lax.rem(me + (n - r), n)


def gather_relatives(x, axis, n):
    known = {0: x}
    if power_of_two(n):
        basis = n - 1
        while basis:
            for r in list(known):
                known[r ^ basis] = lax.ppermute(known[r], axis, relative(n, basis))
            basis //= 2
    else:
        for r in range(1, n):
            known[r] = lax.ppermute(x, axis, relative(n, r))
    return known


def axis_terms(x, axis, n):
    if not power_of_two(n):
        return lax.psum(x, axis), jnp.zeros_like(x)
    bit = 1
    while True:
        got = lax.ppermute(x, axis, relative(n, bit)) if n > 1 else jnp.zeros_like(x)
        bit *= 2
        if bit >= n:
            return x, got
        x = x + got


def column(row, lanes):
    return jnp.transpose(jnp.broadcast_to(row, (lanes, row.shape[1])))


def norm_kernel(members, model_width, starts, rows, meta, square, other, hidden, gain, *outs):
    tokens, features = hidden.shape
    total = square[...] + other[...]
    rstd = column(lax.rsqrt(total / model_width + EPS), LANES)

    def scale(cols):
        return (hidden[:, cols].astype(jnp.float32) * rstd[:, :1]) * gain[:, cols]

    aligned = rows % LANES == 0 and all(s == i * rows for i, s in enumerate(starts))
    for r, out in enumerate(outs):
        member = members(meta[0], r)
        if aligned:
            for at in range(0, rows, LANES):
                cols = pl.ds(pl.multiple_of(member * rows + at, LANES), LANES)
                part = (hidden[:, cols].astype(jnp.float32) * rstd) * gain[:, cols]
                out[:, at : at + LANES] = part.astype(jnp.bfloat16)
        else:
            for i, start in enumerate(starts):

                @pl.when(member == i)
                def _(out=out, start=start):
                    end = min(features, start + rows)
                    part = scale(slice(start, end))
                    if end - start < rows:
                        fill = jnp.zeros((tokens, rows - (end - start)), jnp.float32)
                        part = jnp.concatenate([part, fill], axis=1)
                    out[...] = part.astype(jnp.bfloat16)


def finish_kernel(calls, outer, model_width, meta, square, other, proj, proj_other, hidden, *refs):
    rstd = lax.rsqrt((square[...] + other[...]) / model_width + EPS)
    shift = rstd**3 * (proj[...] + proj_other[...]) / model_width
    rstd, shift = column(rstd, LANES), column(shift, LANES)
    out = refs[-1]
    for relatives, scaled in zip(calls, refs):
        columns = scaled.shape[2]
        for i in range(scaled.shape[0]):
            for at in range(0, columns, LANES):
                cols = pl.ds(at, LANES)
                if relatives is not None:
                    base = relative_index(outer, meta[0], relatives[i]) * columns
                    cols = pl.ds(pl.multiple_of(base + at, LANES), LANES)
                value = hidden[:, cols].astype(jnp.float32)
                grad = scaled[i, :, at : at + LANES] * rstd - value * shift
                out[:, cols] = grad.astype(jnp.bfloat16)


def input_grad_kernel(names, relatives, outer, inner, most, meta, key, grad, hidden, gain, *refs):
    scaled, proj, dense, starts = refs[-4:]
    pieces = [ref for ref in refs[:-4] if ref.dtype == jnp.bfloat16]
    before = [ref for ref in refs[:-4] if ref.dtype == jnp.float32]
    owners = meta.shape[0] - PLACE
    tokens = hidden.shape[0]
    parts = key.shape[1] // LANES
    columns = scaled.shape[2]
    span = columns * parts

    def mark(o, at):
        starts[o] = at
        return at + meta[PLACE + o]

    lax.fori_loop(0, owners, mark, jnp.int32(0))
    slot = lax.broadcasted_iota(jnp.int32, (most, LANES), 0)
    index = 0
    for piece in pieces:
        for i in range(piece.shape[0]):
            r, s = names[index]
            member = relative_index(outer, meta[0], r)
            owner = member * inner + (meta[1] ^ s)
            start = starts[owner]
            if relatives is not None:
                start = start + (relatives.index(r) - member) * span
            rows = pl.ds(start, most)
            new = piece[i].astype(jnp.float32)
            dense[rows, :] = jnp.where(slot < meta[PLACE + owner], new, dense[rows, :])
            index += 1
    step = 256 if columns % 256 == 0 else columns
    total = jnp.zeros((tokens, LANES), jnp.float32)
    for i in range(scaled.shape[0]):
        base = 0
        if relatives is not None:
            base = relative_index(outer, meta[0], relatives[i]) * columns
        for at in range(0, columns, step):
            first = (i * columns + at) * parts
            weight = jnp.concatenate(
                [dense[pl.ds(first + c, step, stride=parts), :] for c in range(parts)], axis=1
            ).astype(jnp.bfloat16)
            cols = pl.ds(at if relatives is None else pl.multiple_of(base + at, LANES), step)
            product = lax.dot_general(
                key[...], weight, (((1,), (1,)), ((), ())), preferred_element_type=jnp.float32
            )
            gained = gain[:, cols] * (grad[:, cols].astype(jnp.float32) + product)
            scaled[i, :, at : at + step] = gained
            terms = gained * hidden[:, cols].astype(jnp.float32)
            for c in range(0, step, LANES):
                total = total + terms[:, c : c + LANES]
    proj[...] = jnp.sum(jnp.transpose(total), axis=0, keepdims=True)
    for ref in before:
        proj[...] += ref[...]


def weight_grad_kernel(sources, inner, group_blocks, most, meta, own, *refs):
    sent, kept, flat, whole = refs[-4:]
    pieces, norms = refs[: len(sources)], refs[len(sources) : -4]
    tokens, width = own.shape
    rows = norms[0].shape[1]
    parts = width // LANES
    whole[:tokens, :] = own[...]
    for place, piece in zip(sources, pieces):
        first = pl.multiple_of(place(meta[2]) * tokens, tokens)
        whole[pl.ds(first, tokens), :] = piece[...]
    step = 256 if rows % 256 == 0 else rows
    for at in range(0, rows, step):
        total = None
        for r, norm in enumerate(norms):
            part = lax.dot_general(
                norm[:, at : at + step],
                whole[r * tokens : (r + 1) * tokens, :],
                (((0,), (0,)), ((), ())),
                preferred_element_type=jnp.float32,
            )
            total = part if total is None else total + part
        for c in range(parts):
            flat[pl.ds(at * parts + c, step, stride=parts), :] = total[:, c * LANES : (c + 1) * LANES]
    outer_index, inner_index = meta[0], meta[1]
    slot = lax.broadcasted_iota(jnp.int32, (most, LANES), 0)
    lead = lax.rem(outer_index * group_blocks, parts)
    for k in range(inner):
        owner = inner_index ^ k

        def add(j, at):
            return at + jnp.where(j < owner, meta[PLACE + outer_index * inner + j], 0)

        start = lax.fori_loop(0, inner, add, lead)
        target = sent if k % 2 else kept
        target[k // 2] = jnp.where(
            slot < meta[PLACE + outer_index * inner + owner], flat[pl.ds(start, most), :], 0.0
        )


def shards(hidden_in, norm_gain, normed_grad, key_grad, weight_blocks, block_count):
    outer, inner, halves = lax.axis_size("gx"), lax.axis_size("gy"), lax.axis_size("gz")
    owners = outer * inner
    most = weight_blocks.shape[2]
    tokens, features = hidden_in.shape
    width = key_grad.shape[1]
    parts = width // LANES
    blocks = features * parts
    group_blocks = (blocks + outer - 1) // outer
    model_width = features * halves
    gx, gy, gz = (lax.axis_index(name) for name in ("gx", "gy", "gz"))
    place = jnp.stack([gx, gy, gz]).astype(jnp.int32)
    meta = jnp.concatenate([place, block_count[0]])

    smem = pl.BlockSpec(memory_space=pltpu.SMEM)
    vmem = pl.BlockSpec(memory_space=pltpu.VMEM)

    def call(kernel, out_shape, scalars, arrays, scratch=(), megabytes=4):
        single = not isinstance(out_shape, tuple)
        return pl.pallas_call(
            kernel,
            out_shape=out_shape,
            in_specs=[smem] * len(scalars) + [vmem] * len(arrays),
            out_specs=vmem if single else (vmem,) * len(out_shape),
            scratch_shapes=list(scratch),
            compiler_params=pltpu.CompilerParams(vmem_limit_bytes=megabytes << 20),
        )(*scalars, *arrays)

    own_blocks = weight_blocks.reshape(most, LANES)
    hidden, gain = hidden_in, norm_gain[None, :]
    hfloat = hidden_in.astype(jnp.float32)
    square = jnp.sum(hfloat * hfloat, axis=1)[None, :]
    found = gather_relatives(own_blocks, "gx", outer)
    order = list(found)
    lots = [lot for lot in (order[:1], order[1:-1], order[-1:]) if lot]
    lots = lots if outer > 1 else [order]

    pieces, names = [], []
    for lot in lots:
        spread = {0: jnp.stack([found[r] for r in lot])}
        bit = inner // 2
        while bit:
            for r in list(spread):
                spread[r ^ bit] = lax.ppermute(spread[r], "gy", relative(inner, bit))
            bit //= 2
        pieces += list(spread.values())
        names += [(r, s) for s in spread for r in lot]

    squares = axis_terms(square, "gz", halves)

    starts = [i * group_blocks // parts for i in range(outer)]
    rows = max(
        ((i + 1) * group_blocks + parts - 1) // parts - starts[i] for i in range(outer)
    )

    def target(i, r):
        return i ^ r if power_of_two(outer) else lax.rem(i + r, outer)

    window = jax.ShapeDtypeStruct((tokens, rows), jnp.bfloat16)
    windows = call(
        functools.partial(norm_kernel, target, model_width, starts, rows),
        (window,) * outer,
        [meta],
        [*squares, hidden, gain],
    )

    sources, key_pieces = [], []

    def bring(place, x, axis, pairs):
        sources.append(place)
        key_pieces.append(lax.ppermute(x, axis, pairs))
        return key_pieces[-1]

    far = range(2, outer)
    shared = power_of_two(outer) and power_of_two(halves) and len(far) == halves
    for r in range(1, 2 if shared else outer):
        bring(lambda g, r=r: r, key_grad, "gx", relative(outer, r))
    if shared:
        pairs = [
            (i * halves + g, (i ^ far[g]) * halves + g) for i in range(outer) for g in range(halves)
        ]
        mine = bring(lambda g: 2 + g, key_grad, ("gx", "gz"), pairs)
        for s in range(1, halves):
            bring(lambda g, s=s: 2 + (g ^ s), mine, "gz", relative(halves, s))
    norms = [windows[0]]
    for r in range(1, outer):
        norms.append(lax.ppermute(windows[r], "gx", relative(outer, r)))

    if group_blocks % parts == 0 and rows * outer == features and rows % LANES == 0 and len(lots) > 2:
        count = sum(r != order[-1] for r, _ in names)
        calls = [order[:-1], order[-1:]]
        parts_of = [(names[:count], pieces[:-inner]), (names[count:], pieces[-inner:])]
    else:
        calls, parts_of = [None], [(names, pieces)]
    scaled, before = [], []
    for relatives, (own_names, own_pieces) in zip(calls, parts_of):
        shape = (1, tokens, features) if relatives is None else (len(relatives), tokens, rows)
        span = shape[0] * shape[2] * parts
        result, proj = call(
            functools.partial(input_grad_kernel, own_names, relatives, outer, inner, most),
            (
                jax.ShapeDtypeStruct(shape, jnp.float32),
                jax.ShapeDtypeStruct((1, tokens), jnp.float32),
            ),
            [meta],
            [key_grad, normed_grad, hidden, gain, *before, *own_pieces],
            [
                pltpu.VMEM((ceil_to(span + most, 8), LANES), jnp.float32),
                pltpu.SMEM((owners,), jnp.int32),
            ],
            megabytes=8,
        )
        scaled.append(result)
        before = [proj]
    projs = axis_terms(proj, "gz", halves)
    hidden_grad = call(
        functools.partial(finish_kernel, calls, outer, model_width),
        jax.ShapeDtypeStruct((tokens, features), jnp.bfloat16),
        [meta],
        [*squares, *projs, hidden, *scaled],
    )

    half = jax.ShapeDtypeStruct((inner // 2, most, LANES), jnp.float32)
    sent, kept = call(
        functools.partial(weight_grad_kernel, sources, inner, group_blocks, most),
        (half, half),
        [meta],
        [key_grad, *key_pieces, *norms],
        [
            pltpu.VMEM((ceil_to(rows * parts + most, 8), LANES), jnp.float32),
            pltpu.VMEM((outer * tokens, width), jnp.bfloat16),
        ],
    )
    bit = 1
    while True:
        got = lax.ppermute(sent, "gy", relative(inner, bit))
        bit *= 2
        if bit == inner:
            break
        sent, kept = kept[1::2] + got[1::2], kept[0::2] + got[0::2]
    owned = (kept + got)[0]
    return (hidden_grad, owned.reshape(1, 1, most, LANES))


def solution(mesh):
    placed = (
        P(("gx", "gy"), "gz"),
        P("gz"),
        P(("gx", "gy"), "gz"),
        P(("gx", "gy"), None),
        P(("gx", "gy"), "gz", None, None),
        P("gz", None),
    )
    return jax.shard_map(
        shards,
        mesh=mesh,
        in_specs=placed,
        out_specs=(P(("gx", "gy"), "gz"), P(("gx", "gy"), "gz", None, None)),
        check_vma=False,
    )
```
